32 devices in a mesh: dev: 16 (over z, y, x), rep: 2 (over core).
Axes of the slice: x: 2, y: 2, z: 4, core: 2. Of those that a mesh axis runs over, the one named last changes fastest.
Arguments:
- tables: bfloat16 [64, 2048, 128], P('dev'), may hold values from -1.5 to 1.5
- bag_rows: int32 [32, 64, 32, 4], P(('rep', 'dev')), parts along dimension 0, may hold values from 0 to 2047
- bag_lengths: int32 [32, 64, 32], P(('rep', 'dev')), parts along dimension 0, may hold values from 1 to 4
- row_counts: int32 [32, 64], P(('rep', 'dev')), parts along dimension 0, may hold values from 1 to 32, as said below
- inverse: int32 [4096, 64], P(('rep', 'dev')), parts along dimension 0, may hold values from 0 to 31
- table_order: int32 [64], replicated, may hold values from 0 to 63, each once
- compress: bfloat16 [16, 64], replicated, may hold values from -0.75 to 0.75
- top_weight: bfloat16 [1024, 512], replicated, may hold values from -0.1875 to 0.1875
- top_bias: float32 [512], replicated, may hold values from -1.8 to 1.8
Outputs:
- ranked: bfloat16 [4096, 512], P(('rep', 'dev')), parts along dimension 0
The draws below stay inside these ranges and needn't reach their ends.
There are 2 independent parts, one for each index of `rep`. The reference program is written for one: setup_inputs(seed, part) draws one part's arguments, and reference() takes and returns one part's arrays. A program takes and returns all parts, laid end to end along the dimension named above; an argument that names none is the same for every part. Nothing has to cross between parts.
Inputs may be any that keep to these rules, and one draw needn't show every extreme that they name: `row_counts`: for every sample device and every aligned group of 4 consecutive slots the counts sum to at most 80; a count of 32 and a group sum of 80 occur in every draw.
All inputs are finite; a program needn't handle non-finite values.
Results may differ from the reference program's by a relative error of at most 0.0062.
Values may be sent and summed in bfloat16 or wider, within the bound.
A program may use at most 128 MiB of HBM per device.

```python
import math
import jax
import jax.numpy as jnp
import numpy as np
from jax import lax

WIDTH = 128
VOCABULARY = 2048
TABLES_DEV = 4
TABLES = 64
BATCH_DEV = 128
BATCH = 2048
ROWS_MOST = 32
PACK_ROOM = 80
POOLING = 4
COMPRESSED = 16
TOP_UNITS = 512
N_DEV = 16


def draw_row_counts(key, part):
    first_key = jax.random.fold_in(key, 11)
    second_key = jax.random.fold_in(key, 12)
    third_key = jax.random.fold_in(key, 13)
    raw_counts = jax.random.randint(first_key, (N_DEV, N_DEV, TABLES_DEV), 1, ROWS_MOST + 1)
    group_total = jnp.sum(raw_counts, axis=2, keepdims=True)
    shrunk = 1 + (raw_counts - 1) * (PACK_ROOM - TABLES_DEV) // jnp.maximum(group_total - TABLES_DEV, 1)
    scaled = jnp.where(group_total > PACK_ROOM, shrunk, raw_counts)
    shift_value = jax.random.randint(second_key, (), 0, 5)
    device_range = jnp.arange(N_DEV, dtype=jnp.int32)[:, None]
    group_range = jnp.arange(N_DEV, dtype=jnp.int32)[None, :]
    forced = (device_range * 3 + group_range + shift_value) % 5 == 0
    leader = jax.random.randint(third_key, (N_DEV, N_DEV), 0, TABLES_DEV)
    remainder = PACK_ROOM - ROWS_MOST
    share_value = remainder // (TABLES_DEV - 1)
    last_value = remainder - (TABLES_DEV - 2) * share_value
    member = jnp.arange(TABLES_DEV, dtype=jnp.int32)[None, None, :]
    ranking = (member - leader[..., None]) % TABLES_DEV
    filled = jnp.where(ranking == 0, ROWS_MOST, jnp.where(ranking == TABLES_DEV - 1, last_value, share_value))
    result = jnp.where(forced[..., None], filled, scaled)
    return result.reshape(N_DEV, TABLES).astype(jnp.int32)


def with_ends(values, rng, smallest, largest):
    longest = values.shape.index(max(values.shape))
    spots = []
    for shift in (0, 1):
        where = [jax.random.randint(jax.random.fold_in(rng, axis), (), 0, length) for axis, length in enumerate(values.shape)]
        where[longest] = (where[longest] + shift) % values.shape[longest]
        spots.append(tuple(where))
    return values.at[spots[0]].set(smallest).at[spots[1]].set(largest)


def levels(own_key, dims, cuts, least, top_value):
    factor_of, own = 1.0, jax.random.fold_in(own_key, 6)
    for axis_at, blocks in cuts:
        heights = jnp.exp(jax.random.uniform(jax.random.fold_in(own, axis_at), (blocks,), jnp.float32, least / len(cuts), top_value / len(cuts)))
        factor_of = factor_of * jnp.repeat(heights, dims[axis_at] // blocks).reshape([-1 if axis == axis_at else 1 for axis in range(len(dims))])
    return factor_of


def rank_bounds(count, skew):
    weights = [(1 << 20) // math.isqrt(standing ** skew) + 1 for standing in range(1, count + 1)]
    width = 1 + sum(weights) // (1 << 30)
    return np.cumsum(np.array([max(1, weight // width) for weight in weights]))


def ranked_ids(stream_key, extent, number_of, skew):
    listing = rank_bounds(number_of, skew)
    pick = jax.random.randint(jax.random.fold_in(stream_key, 1), extent, 0, int(listing[number_of - 1]))
    rank = jnp.searchsorted(jnp.asarray(listing, jnp.int32), pick, side="right")
    return jax.random.permutation(jax.random.fold_in(stream_key, 2), number_of)[rank].astype(jnp.int32)


def gaussian(own_key, dims, scale, bound, split=(), kind=jnp.bfloat16):
    drawn = scale * jax.random.normal(own_key, dims, jnp.float32)
    if split:
        drawn = drawn * levels(own_key, dims, split, -0.22, 0.18)
    return jnp.clip(drawn, -bound, bound).astype(kind)


def setup_inputs(seed: int = 0, part: int = 0) -> dict:
    seeds = jax.random.split(jax.random.key(seed), 10)
    part_keys = jax.random.split(jax.random.fold_in(seeds[9], part), 10)
    tables = gaussian(seeds[0], (TABLES, VOCABULARY, WIDTH), 0.25, 1.5, ((0, 16),))
    bag_rows = with_ends(ranked_ids(part_keys[1], (N_DEV, TABLES, ROWS_MOST, POOLING), VOCABULARY, 2), jax.random.fold_in(part_keys[1], 3), 0, VOCABULARY - 1).astype(jnp.int32)
    bag_lengths = with_ends(jax.random.randint(part_keys[2], (N_DEV, TABLES, ROWS_MOST), 1, POOLING + 1), jax.random.fold_in(part_keys[2], 1), 1, POOLING).astype(jnp.int32)
    row_counts = draw_row_counts(jax.random.fold_in(jax.random.fold_in(seeds[9], part), 71), part)
    inverse = with_ends(jax.random.randint(part_keys[4], (BATCH, TABLES), 0, ROWS_MOST), jax.random.fold_in(part_keys[4], 1), 0, ROWS_MOST - 1).astype(jnp.int32)
    table_order = jax.random.permutation(seeds[5], TABLES).astype(jnp.int32)
    compress = gaussian(seeds[6], (COMPRESSED, TABLES), TABLES ** -0.5, 0.75)
    top_weight = gaussian(seeds[7], (TABLES * COMPRESSED, TOP_UNITS), (TABLES * COMPRESSED) ** -0.5, 0.1875)
    top_bias = gaussian(seeds[8], (TOP_UNITS,), 0.3, 1.8, (), jnp.float32)
    return {"tables": tables, "bag_rows": bag_rows, "bag_lengths": bag_lengths, "row_counts": row_counts, "inverse": inverse, "table_order": table_order, "compress": compress, "top_weight": top_weight, "top_bias": top_bias}


def pool_rows(tables, rows_here, lengths_here):
    gathered = jax.vmap(lambda one_table, one_bag: jnp.take(one_table, one_bag, axis=0))(tables, rows_here)
    active = jnp.arange(rows_here.shape[2], dtype=jnp.int32)[None, None, :] < lengths_here[..., None]
    summed = jnp.sum(jnp.where(active[..., None], gathered.astype(jnp.float32), jnp.zeros((), jnp.float32)), axis=2)
    return summed.astype(jnp.bfloat16)


def interact(features, compress, top_weight, top_bias):
    mixed = jnp.einsum("kf,bfe->bke", compress.astype(jnp.float32), features.astype(jnp.float32)).astype(jnp.bfloat16)
    pairwise = jnp.einsum("bfe,bke->bfk", features.astype(jnp.float32), mixed.astype(jnp.float32)).astype(jnp.bfloat16)
    hidden_pre = jnp.dot(pairwise.reshape(pairwise.shape[0], -1), top_weight, preferred_element_type=jnp.float32) + top_bias
    return jnp.maximum(hidden_pre, jnp.zeros((), jnp.float32)).astype(jnp.bfloat16)


def reference(tables, bag_rows, bag_lengths, row_counts, inverse, table_order, compress, top_weight, top_bias):
    slot_range = jnp.arange(TABLES, dtype=jnp.int32)
    matches = table_order[:, None] == slot_range[None, :]
    slot_of = jnp.sum(jnp.where(matches, slot_range[:, None], 0), axis=0).astype(jnp.int32)

    def one_device(device):
        rows_here = lax.dynamic_index_in_dim(bag_rows, device, 0, keepdims=False)
        lengths_here = lax.dynamic_index_in_dim(bag_lengths, device, 0, keepdims=False)
        counts_here = lax.dynamic_index_in_dim(row_counts, device, 0, keepdims=False)
        inverse_here = lax.dynamic_slice_in_dim(inverse, (device * BATCH_DEV).astype(jnp.int32), BATCH_DEV, 0)
        pooled = pool_rows(tables, rows_here, lengths_here)
        flat_rows = pooled.reshape(-1, WIDTH)
        positions = (slot_of[None, :] * ROWS_MOST + inverse_here).astype(jnp.int32)
        gathered = jnp.take(flat_rows, positions, axis=0)
        present = inverse_here < counts_here[slot_of][None, :]
        features = jnp.where(present[..., None], gathered, jnp.zeros((), jnp.bfloat16))
        return interact(features, compress, top_weight, top_bias)

    result = lax.map(one_device, jnp.arange(N_DEV, dtype=jnp.int32))
    return result.reshape(BATCH, TOP_UNITS)
```

```python
import functools

import jax
import jax.numpy as jnp
from jax import lax
from jax.experimental import pallas as pl
from jax.experimental.pallas import tpu as pltpu
from jax.sharding import PartitionSpec as P

F32 = jnp.float32
BF16 = jnp.bfloat16


def exchange_kernel(
    n, most, bags_ref, tables_ref, rows_ref,
    tab16, tab32, ids_out, ids_vm, ids_in, pooled, staging,
    tab_sem, id_send, id_recv, smem_sem, row_send, row_recv, own_sem,
):
    me = lax.axis_index("dev")
    tabs, vocab, width = tables_ref.shape
    spread = bags_ref.shape[0]
    pooling = spread // most
    zero_row = tabs * vocab

    table_copy = pltpu.make_async_copy(tables_ref, tab16, tab_sem)
    table_copy.start()
    barrier = pltpu.get_barrier_semaphore()

    def greet(i, carry):
        pl.semaphore_signal(barrier, inc=1, device_id={"dev": lax.rem(me + i, n)})
        return carry

    lax.fori_loop(1, n, greet, 0)

    index = bags_ref[...].T
    for g in range(n):
        ids_out[g] = index[g * tabs:(g + 1) * tabs]

    pl.semaphore_wait(barrier, n - 1)

    def id_copy(i):
        peer = lax.rem(me + i, n)
        return pltpu.make_async_remote_copy(
            src_ref=ids_out.at[peer], dst_ref=ids_vm.at[me],
            send_sem=id_send.at[peer], recv_sem=id_recv.at[me],
            device_id={"dev": peer},
        )

    def id_arrival(source):
        return pltpu.make_async_remote_copy(
            src_ref=ids_out.at[source], dst_ref=ids_vm.at[source],
            send_sem=id_send.at[source], recv_sem=id_recv.at[source],
            device_id={"dev": source},
        )

    def offset(j):
        half = (j + 1) // 2
        return n // 2 + jnp.where(j % 2 == 1, half, -half)

    def send_ids(j, carry):
        id_copy(offset(j)).start()
        return carry

    lax.fori_loop(0, n - 1, send_ids, 0)

    table_copy.wait()
    tab32[pl.ds(zero_row, 8), :] = jnp.zeros((8, width), F32)
    step = 256

    def widen(i, carry):
        for t in range(tabs):
            base = pl.multiple_of(i * step, step)
            tab32[pl.ds(t * vocab + base, step), :] = tab16[t, pl.ds(base, step), :].astype(F32)
        return carry

    lax.fori_loop(0, vocab // step, widen, 0)

    def pool(source_ref, store):
        def eight(i, carry):
            for t in range(tabs):
                parts = []
                for r in range(8):
                    total = None
                    for p in range(pooling):
                        at = source_ref[t, (i * 8 + r) * pooling + p]
                        row = tab32[pl.ds(at, 1), :]
                        total = row if total is None else total + row
                    pooled[pl.ds(t * most + i * 8 + r, 1), :] = total
            return carry

        lax.fori_loop(0, most // 8, eight, 0)
        store(pooled[...].astype(BF16))

    def row_copy(peer):
        return pltpu.make_async_remote_copy(
            src_ref=staging.at[peer], dst_ref=rows_ref.at[me],
            send_sem=row_send.at[peer], recv_sem=row_recv.at[me],
            device_id={"dev": peer},
        )

    def serve(j, carry):
        peer = lax.rem(me + offset(j), n)
        id_arrival(peer).wait_recv()
        down = pltpu.make_async_copy(ids_vm.at[peer], ids_in, smem_sem)
        down.start()
        down.wait()

        def store(value):
            staging[peer] = value

        pool(ids_in, store)
        row_copy(peer).start()
        return carry

    lax.fori_loop(0, n - 1, serve, 0)

    down = pltpu.make_async_copy(ids_out.at[me], ids_in, smem_sem)
    down.start()
    down.wait()

    def store_own(value):
        rows_ref[me] = value

    pool(ids_in, store_own)

    def finish(i, carry):
        peer = lax.rem(me + i, n)
        id_copy(i).wait_send()
        row_copy(peer).wait_send()
        pltpu.make_async_remote_copy(
            src_ref=staging.at[peer], dst_ref=rows_ref.at[peer],
            send_sem=row_send.at[peer], recv_sem=row_recv.at[peer],
            device_id={"dev": peer},
        ).wait_recv()
        return carry

    lax.fori_loop(1, n, finish, 0)


def exchange(n, most, bags, tables):
    tabs, vocab, width = tables.shape
    spread, slots = bags.shape
    block = tabs * most
    vmem = pl.BlockSpec(memory_space=pltpu.VMEM)
    return pl.pallas_call(
        functools.partial(exchange_kernel, n, most),
        out_shape=jax.ShapeDtypeStruct((n, block, width), BF16),
        in_specs=[vmem, pl.BlockSpec(memory_space=pl.ANY)],
        out_specs=vmem,
        scratch_shapes=[
            pltpu.VMEM(tables.shape, BF16),
            pltpu.VMEM((tabs * vocab + 8, width), F32),
            pltpu.VMEM((n, tabs, spread), jnp.int32),
            pltpu.VMEM((n, tabs, spread), jnp.int32),
            pltpu.SMEM((tabs, spread), jnp.int32),
            pltpu.VMEM((block, width), F32),
            pltpu.VMEM((n, block, width), BF16),
            pltpu.SemaphoreType.DMA,
            pltpu.SemaphoreType.DMA((n,)),
            pltpu.SemaphoreType.DMA((n,)),
            pltpu.SemaphoreType.DMA,
            pltpu.SemaphoreType.DMA((n,)),
            pltpu.SemaphoreType.DMA((n,)),
            pltpu.SemaphoreType.DMA,
        ],
        compiler_params=pltpu.CompilerParams(
            collective_id=0, has_side_effects=True, vmem_limit_bytes=48 << 20
        ),
        name="exchange",
    )(bags, tables)


def interact_kernel(
    rows_ref, inv_ref, order_ref, counts_ref, compress_ref, weight_ref, bias_ref, out_ref,
    sel, spread_c, mask, mixed, pairs,
):
    features, samples = inv_ref.shape
    mixes = compress_ref.shape[0]
    total, width = rows_ref.shape
    most = total // features
    per = 8
    span = per * most
    inv = inv_ref[...].astype(F32).T.astype(BF16)
    comp = compress_ref[...]

    def select(c, carry):
        lane = lax.broadcasted_iota(jnp.int32, (1, span), 1)
        slot, unit = lane // most, lane % most
        order_row = jnp.zeros((1, span), jnp.int32)
        count_row = jnp.zeros((1, span), jnp.int32)
        row_u = lax.broadcasted_iota(jnp.int32, (most, samples), 0)
        for i in range(per):
            s = c * per + i
            f, count = order_ref[s], counts_ref[s]
            order_row = jnp.where(slot == i, f, order_row)
            count_row = jnp.where(slot == i, count, count_row)
            wanted = inv_ref[pl.ds(f, 1), :]
            hit = jnp.logical_and(row_u == wanted, row_u < count)
            mask[pl.ds(pl.multiple_of(s * most, most), most), :] = jnp.where(hit, 1.0, 0.0)
        target = jnp.where(unit < count_row, unit, -1).astype(F32)
        feature = lax.broadcasted_iota(jnp.int32, (features, span), 0)
        one_hot = jnp.where(feature == order_row, 1.0, 0.0).astype(BF16)
        inv_all = jnp.dot(inv, one_hot, preferred_element_type=F32)
        columns = pl.ds(pl.multiple_of(c * span, span), span)
        sel[:, columns] = jnp.where(inv_all == target, 1.0, 0.0).astype(BF16)
        spread_c[:, columns] = jnp.dot(comp, one_hot, preferred_element_type=F32)
        return carry

    lax.fori_loop(0, features // per, select, 0)

    deep = min(total, 2048)

    def mix(k, carry):
        acc = jnp.zeros((samples, width), F32)

        def part(q, acc):
            columns = pl.ds(pl.multiple_of(q * deep, deep), deep)
            scaled = sel[:, columns] * spread_c[pl.ds(k, 1), columns].astype(BF16)
            return acc + jnp.dot(scaled, rows_ref[columns, :], preferred_element_type=F32)

        if total == deep:
            acc = part(0, acc)
        else:
            acc = lax.fori_loop(0, total // deep, part, acc)
        mixed[pl.ds(pl.multiple_of(k * samples, samples), samples), :] = acc.astype(BF16)
        return carry

    lax.fori_loop(0, mixes, mix, 0)

    pair = 2

    def inner(j, carry):
        c8, kp = j // (mixes // pair), j % (mixes // pair)
        wanted = mixed[pl.ds(pl.multiple_of(kp * pair * samples, samples), pair * samples), :]
        for i in range(per):
            c = c8 * per + i
            at = pl.ds(pl.multiple_of(c * span, span), span)
            product = lax.dot_general(
                rows_ref[at, :], wanted, (((1,), (1,)), ((), ())), preferred_element_type=F32
            )
            chosen = mask[at, :]
            for h in range(pair):
                kept = product[:, h * samples:(h + 1) * samples] * chosen
                summed = jnp.sum(kept.reshape(per, most, samples), axis=1)
                for s in range(per):
                    f = order_ref[c * per + s]
                    pairs[pl.ds(f * mixes + kp * pair + h, 1), :] = summed[s:s + 1, :]
        return carry

    lax.fori_loop(0, features // (per * per) * (mixes // pair), inner, 0)

    depth = min(features * mixes, 1024)
    hidden = jnp.zeros(out_ref.shape, F32) + bias_ref[...]

    def top(q, hidden):
        at = pl.ds(pl.multiple_of(q * depth, depth), depth)
        return hidden + lax.dot_general(
            pairs[at, :].astype(BF16), weight_ref[at, :], (((0,), (0,)), ((), ())),
            preferred_element_type=F32,
        )

    if depth == features * mixes:
        hidden = top(0, hidden)
    else:
        hidden = lax.fori_loop(0, features * mixes // depth, top, hidden)
    out_ref[...] = jnp.maximum(hidden, 0.0).astype(BF16)


def interact(rows, inv, order, counts, compress, weight, bias):
    features, samples = inv.shape
    mixes = compress.shape[0]
    total, width = rows.shape
    vmem = pl.BlockSpec(memory_space=pltpu.VMEM)
    smem = pl.BlockSpec(memory_space=pltpu.SMEM)
    return pl.pallas_call(
        interact_kernel,
        out_shape=jax.ShapeDtypeStruct((samples, weight.shape[1]), BF16),
        in_specs=[vmem, vmem, smem, smem, vmem, vmem, vmem],
        out_specs=vmem,
        scratch_shapes=[
            pltpu.VMEM((samples, total), BF16),
            pltpu.VMEM((mixes, total), F32),
            pltpu.VMEM((total, samples), F32),
            pltpu.VMEM((mixes * samples, width), BF16),
            pltpu.VMEM((features * mixes, samples), F32),
        ],
        compiler_params=pltpu.CompilerParams(vmem_limit_bytes=60 << 20),
        name="interact",
    )(rows, inv, order, counts, compress, weight, bias)


def shards(
    n, tables, bag_rows, bag_lengths, row_counts, inverse, table_order, compress, top_weight, top_bias
):
    _, slots, most, pooling = bag_rows.shape
    tabs, vocab, width = tables.shape
    local = (jnp.arange(slots, dtype=jnp.int32) % tabs) * vocab
    active = jnp.arange(pooling, dtype=jnp.int32)[:, None] < bag_lengths[0].T[:, None, :]
    index = jnp.where(active, bag_rows[0].transpose(1, 2, 0) + local, tabs * vocab)
    rows = exchange(n, most, index.reshape(most * pooling, slots), tables)
    return interact(
        rows.reshape(slots * most, width), inverse.T, table_order, row_counts[0],
        compress, top_weight, top_bias.reshape(1, -1),
    )


def solution(mesh):
    return jax.shard_map(
        functools.partial(shards, mesh.shape["dev"]),
        mesh=mesh,
        in_specs=(
            P("dev", None, None),
            P(("rep", "dev"), None, None, None),
            P(("rep", "dev"), None, None),
            P(("rep", "dev"), None),
            P(("rep", "dev"), None),
            P(),
            P(),
            P(),
            P(),
        ),
        out_specs=P(("rep", "dev"), None),
        check_vma=False,
    )
```

```python
import functools

import jax
import jax.numpy as jnp
from jax import lax
from jax.experimental import pallas as pl
from jax.experimental.pallas import tpu as pltpu
from jax.sharding import PartitionSpec as P

F32 = jnp.float32
BF16 = jnp.bfloat16


def exchange_kernel(
    n, most, bags_ref, tables_ref, rows_ref,
    tab16, tab32, ids_out, ids_in, pooled, staging,
    tab_sem, id_send, id_recv, smem_sem, row_send, row_recv,
):
    me = lax.axis_index("dev")
    tabs, vocab, width = tables_ref.shape
    spread = bags_ref.shape[0]
    pooling = spread // most
    zero_row = tabs * vocab

    table_copy = pltpu.make_async_copy(tables_ref, tab16, tab_sem)
    table_copy.start()
    barrier = pltpu.get_barrier_semaphore()

    def greet(i, carry):
        pl.semaphore_signal(barrier, inc=1, device_id={"dev": lax.rem(me + i, n)})
        return carry

    lax.fori_loop(1, n, greet, 0)

    index = bags_ref[...].T
    for g in range(n):
        ids_out[g] = index[g * tabs:(g + 1) * tabs]

    pl.semaphore_wait(barrier, n - 1)

    def id_copy(i):
        peer = lax.rem(me + i, n)
        return pltpu.make_async_remote_copy(
            src_ref=ids_out.at[peer], dst_ref=ids_in.at[me],
            send_sem=id_send.at[peer], recv_sem=id_recv.at[me],
            device_id={"dev": peer},
        )

    def id_arrival(source):
        return pltpu.make_async_remote_copy(
            src_ref=ids_out.at[source], dst_ref=ids_in.at[source],
            send_sem=id_send.at[source], recv_sem=id_recv.at[source],
            device_id={"dev": source},
        )

    def offset(j):
        half = (j + 1) // 2
        return n // 2 + jnp.where(j % 2 == 1, half, -half)

    def send_ids(j, carry):
        id_copy(offset(j)).start()
        return carry

    lax.fori_loop(0, n - 1, send_ids, 0)

    own_ids = pltpu.make_async_copy(ids_out.at[me], ids_in.at[me], smem_sem)
    own_ids.start()
    table_copy.wait()
    tab32[pl.ds(zero_row, 8), :] = jnp.zeros((8, width), F32)
    step = 256

    def widen(i, carry):
        for t in range(tabs):
            base = pl.multiple_of(i * step, step)
            tab32[pl.ds(t * vocab + base, step), :] = tab16[t, pl.ds(base, step), :].astype(F32)
        return carry

    lax.fori_loop(0, vocab // step, widen, 0)

    def pool(source, store):
        def one_table(t, carry):
            at_table = pl.multiple_of(t * most, most)
            for r in range(most):
                total = None
                for p in range(pooling):
                    row = tab32[pl.ds(ids_in[source, t, r * pooling + p], 1), :]
                    total = row if total is None else total + row
                pooled[pl.ds(at_table + r, 1), :] = total
            return carry

        lax.fori_loop(0, tabs, one_table, 0)
        store(pooled[...].astype(BF16))

    def row_copy(peer):
        return pltpu.make_async_remote_copy(
            src_ref=staging.at[peer], dst_ref=rows_ref.at[me],
            send_sem=row_send.at[peer], recv_sem=row_recv.at[me],
            device_id={"dev": peer},
        )

    def serve(j, carry):
        peer = lax.rem(me + offset(j), n)
        id_arrival(peer).wait_recv()

        def store(value):
            staging[peer] = value

        pool(peer, store)
        row_copy(peer).start()
        return carry

    lax.fori_loop(0, n - 1, serve, 0)

    own_ids.wait()

    def store_own(value):
        rows_ref[me] = value

    pool(me, store_own)

    def finish(i, carry):
        peer = lax.rem(me + i, n)
        id_copy(i).wait_send()
        row_copy(peer).wait_send()
        pltpu.make_async_remote_copy(
            src_ref=staging.at[peer], dst_ref=rows_ref.at[peer],
            send_sem=row_send.at[peer], recv_sem=row_recv.at[peer],
            device_id={"dev": peer},
        ).wait_recv()
        return carry

    lax.fori_loop(1, n, finish, 0)


def exchange(n, most, bags, tables):
    tabs, vocab, width = tables.shape
    spread, slots = bags.shape
    block = tabs * most
    vmem = pl.BlockSpec(memory_space=pltpu.VMEM)
    return pl.pallas_call(
        functools.partial(exchange_kernel, n, most),
        out_shape=jax.ShapeDtypeStruct((n, block, width), BF16),
        in_specs=[vmem, pl.BlockSpec(memory_space=pl.ANY)],
        out_specs=vmem,
        scratch_shapes=[
            pltpu.VMEM(tables.shape, BF16),
            pltpu.VMEM((tabs * vocab + 8, width), F32),
            pltpu.VMEM((n, tabs, spread), jnp.int32),
            pltpu.SMEM((n, tabs, spread), jnp.int32),
            pltpu.VMEM((block, width), F32),
            pltpu.VMEM((n, block, width), BF16),
            pltpu.SemaphoreType.DMA,
            pltpu.SemaphoreType.DMA((n,)),
            pltpu.SemaphoreType.DMA((n,)),
            pltpu.SemaphoreType.DMA,
            pltpu.SemaphoreType.DMA((n,)),
            pltpu.SemaphoreType.DMA((n,)),
        ],
        compiler_params=pltpu.CompilerParams(
            collective_id=0, has_side_effects=True, vmem_limit_bytes=62 << 20
        ),
        name="exchange",
    )(bags, tables)


def interact_kernel(
    rows_ref, inv_ref, order_ref, counts_ref, compress_ref, weight_ref, bias_ref, out_ref,
    sel, spread_c, mask, mixed, pairs,
):
    features, samples = inv_ref.shape
    mixes = compress_ref.shape[0]
    total, width = rows_ref.shape
    most = total // features
    per = 8
    span = per * most
    inv = inv_ref[...].astype(F32).T.astype(BF16)
    comp = compress_ref[...]

    def select(c, carry):
        lane = lax.broadcasted_iota(jnp.int32, (1, span), 1)
        slot, unit = lane // most, lane % most
        order_row = jnp.zeros((1, span), jnp.int32)
        count_row = jnp.zeros((1, span), jnp.int32)
        row_u = lax.broadcasted_iota(jnp.int32, (most, samples), 0)
        for i in range(per):
            s = c * per + i
            f, count = order_ref[s], counts_ref[s]
            order_row = jnp.where(slot == i, f, order_row)
            count_row = jnp.where(slot == i, count, count_row)
            wanted = inv_ref[pl.ds(f, 1), :]
            hit = jnp.logical_and(row_u == wanted, row_u < count)
            mask[pl.ds(pl.multiple_of(s * most, most), most), :] = jnp.where(hit, 1.0, 0.0)
        target = jnp.where(unit < count_row, unit, -1).astype(F32)
        feature = lax.broadcasted_iota(jnp.int32, (features, span), 0)
        one_hot = jnp.where(feature == order_row, 1.0, 0.0).astype(BF16)
        inv_all = jnp.dot(inv, one_hot, preferred_element_type=F32)
        columns = pl.ds(pl.multiple_of(c * span, span), span)
        sel[:, columns] = jnp.where(inv_all == target, 1.0, 0.0).astype(BF16)
        spread_c[:, columns] = jnp.dot(comp, one_hot, preferred_element_type=F32)
        return carry

    lax.fori_loop(0, features // per, select, 0)

    deep = min(total, 2048)

    def mix(k, carry):
        acc = jnp.zeros((samples, width), F32)

        def part(q, acc):
            columns = pl.ds(pl.multiple_of(q * deep, deep), deep)
            scaled = sel[:, columns] * spread_c[pl.ds(k, 1), columns].astype(BF16)
            return acc + jnp.dot(scaled, rows_ref[columns, :], preferred_element_type=F32)

        if total == deep:
            acc = part(0, acc)
        else:
            acc = lax.fori_loop(0, total // deep, part, acc)
        mixed[pl.ds(pl.multiple_of(k * samples, samples), samples), :] = acc.astype(BF16)
        return carry

    lax.fori_loop(0, mixes, mix, 0)

    pair = 2

    def inner(j, carry):
        c8, kp = j // (mixes // pair), j % (mixes // pair)
        wanted = mixed[pl.ds(pl.multiple_of(kp * pair * samples, samples), pair * samples), :]
        for i in range(per):
            c = c8 * per + i
            at = pl.ds(pl.multiple_of(c * span, span), span)
            product = lax.dot_general(
                rows_ref[at, :], wanted, (((1,), (1,)), ((), ())), preferred_element_type=F32
            )
            chosen = mask[at, :]
            for h in range(pair):
                kept = product[:, h * samples:(h + 1) * samples] * chosen
                summed = jnp.sum(kept.reshape(per, most, samples), axis=1)
                for s in range(per):
                    f = order_ref[c * per + s]
                    pairs[pl.ds(f * mixes + kp * pair + h, 1), :] = summed[s:s + 1, :]
        return carry

    lax.fori_loop(0, features // (per * per) * (mixes // pair), inner, 0)

    depth = min(features * mixes, 1024)
    hidden = jnp.zeros(out_ref.shape, F32) + bias_ref[...]

    def top(q, hidden):
        at = pl.ds(pl.multiple_of(q * depth, depth), depth)
        return hidden + lax.dot_general(
            pairs[at, :].astype(BF16), weight_ref[at, :], (((0,), (0,)), ((), ())),
            preferred_element_type=F32,
        )

    if depth == features * mixes:
        hidden = top(0, hidden)
    else:
        hidden = lax.fori_loop(0, features * mixes // depth, top, hidden)
    out_ref[...] = jnp.maximum(hidden, 0.0).astype(BF16)


def interact(rows, inv, order, counts, compress, weight, bias):
    features, samples = inv.shape
    mixes = compress.shape[0]
    total, width = rows.shape
    held = rows.size + weight.size + samples * total + 2 * (mixes + samples) * total
    held += mixes * samples * width + 2 * features * mixes * samples
    vmem = pl.BlockSpec(memory_space=pltpu.VMEM)
    smem = pl.BlockSpec(memory_space=pltpu.SMEM)
    return pl.pallas_call(
        interact_kernel,
        out_shape=jax.ShapeDtypeStruct((samples, weight.shape[1]), BF16),
        in_specs=[vmem, vmem, smem, smem, vmem, vmem, vmem],
        out_specs=vmem,
        scratch_shapes=[
            pltpu.VMEM((samples, total), BF16),
            pltpu.VMEM((mixes, total), F32),
            pltpu.VMEM((total, samples), F32),
            pltpu.VMEM((mixes * samples, width), BF16),
            pltpu.VMEM((features * mixes, samples), F32),
        ],
        compiler_params=pltpu.CompilerParams(vmem_limit_bytes=min(60 << 20, (8 << 20) + 3 * held)),
        name="interact",
    )(rows, inv, order, counts, compress, weight, bias)


def shards(
    n, tables, bag_rows, bag_lengths, row_counts, inverse, table_order, compress, top_weight, top_bias
):
    _, slots, most, pooling = bag_rows.shape
    tabs, vocab, width = tables.shape
    local = (jnp.arange(slots, dtype=jnp.int32) % tabs) * vocab
    active = jnp.arange(pooling, dtype=jnp.int32)[:, None] < bag_lengths[0].T[:, None, :]
    index = jnp.where(active, bag_rows[0].transpose(1, 2, 0) + local, tabs * vocab)
    rows = exchange(n, most, index.reshape(most * pooling, slots), tables)
    return interact(
        rows.reshape(slots * most, width), inverse.T, table_order, row_counts[0],
        compress, top_weight, top_bias.reshape(1, -1),
    )


def solution(mesh):
    return jax.shard_map(
        functools.partial(shards, mesh.shape["dev"]),
        mesh=mesh,
        in_specs=(
            P("dev", None, None),
            P(("rep", "dev"), None, None, None),
            P(("rep", "dev"), None, None),
            P(("rep", "dev"), None),
            P(("rep", "dev"), None),
            P(),
            P(),
            P(),
            P(),
        ),
        out_specs=P(("rep", "dev"), None),
        check_vma=False,
    )
```

```python
import functools

import jax
import jax.numpy as jnp
from jax import lax
from jax.experimental import pallas as pl
from jax.experimental.pallas import tpu as pltpu
from jax.sharding import PartitionSpec as P

F32 = jnp.float32
BF16 = jnp.bfloat16


def select_samples(
    most, inv_ref, order_ref, counts_ref, compress_ref, sel, spread_c, mask
):
    features, samples = inv_ref.shape
    per = 8
    span = per * most
    inv = inv_ref[...].astype(F32).T.astype(BF16)
    comp = compress_ref[...]

    def select(c, carry):
        lane = lax.broadcasted_iota(jnp.int32, (1, span), 1)
        slot, unit = lane // most, lane % most
        order_row = jnp.zeros((1, span), jnp.int32)
        count_row = jnp.zeros((1, span), jnp.int32)
        row_u = lax.broadcasted_iota(jnp.int32, (most, samples), 0)
        for i in range(per):
            s = c * per + i
            f, count = order_ref[s], counts_ref[s]
            order_row = jnp.where(slot == i, f, order_row)
            count_row = jnp.where(slot == i, count, count_row)
            wanted = inv_ref[pl.ds(f, 1), :]
            hit = jnp.logical_and(row_u == wanted, row_u < count)
            mask[pl.ds(pl.multiple_of(s * most, most), most), :] = jnp.where(hit, 1.0, 0.0)
        target = jnp.where(unit < count_row, unit, -1).astype(F32)
        feature = lax.broadcasted_iota(jnp.int32, (features, span), 0)
        one_hot = jnp.where(feature == order_row, 1.0, 0.0).astype(BF16)
        inv_all = jnp.dot(inv, one_hot, preferred_element_type=F32)
        columns = pl.ds(pl.multiple_of(c * span, span), span)
        sel[:, columns] = jnp.where(inv_all == target, 1.0, 0.0).astype(BF16)
        spread_c[:, columns] = jnp.dot(comp, one_hot, preferred_element_type=F32)
        return carry

    lax.fori_loop(0, features // per, select, 0)


def exchange_kernel(
    n, most, bags_ref, tables_ref, inv_ref, order_ref, counts_ref, compress_ref,
    rows_ref, sel, spread_c, mask,
    tab16, tab32, ids_out, ids_in, pooled, staging,
    tab_sem, id_send, id_recv, smem_sem, row_send, row_recv,
):
    me = lax.axis_index("dev")
    tabs, vocab, width = tables_ref.shape
    spread = bags_ref.shape[0]
    pooling = spread // most
    zero_row = tabs * vocab

    table_copy = pltpu.make_async_copy(tables_ref, tab16, tab_sem)
    table_copy.start()
    barrier = pltpu.get_barrier_semaphore()

    def greet(i, carry):
        pl.semaphore_signal(barrier, inc=1, device_id={"dev": lax.rem(me + i, n)})
        return carry

    lax.fori_loop(1, n, greet, 0)

    index = bags_ref[...].T
    for g in range(n):
        ids_out[g] = index[g * tabs:(g + 1) * tabs]

    pl.semaphore_wait(barrier, n - 1)

    def id_copy(i):
        peer = lax.rem(me + i, n)
        return pltpu.make_async_remote_copy(
            src_ref=ids_out.at[peer], dst_ref=ids_in.at[me],
            send_sem=id_send.at[peer], recv_sem=id_recv.at[me],
            device_id={"dev": peer},
        )

    def id_arrival(source):
        return pltpu.make_async_remote_copy(
            src_ref=ids_out.at[source], dst_ref=ids_in.at[source],
            send_sem=id_send.at[source], recv_sem=id_recv.at[source],
            device_id={"dev": source},
        )

    def offset(j):
        half = (j + 1) // 2
        return n // 2 + jnp.where(j % 2 == 1, half, -half)

    def send_ids(j, carry):
        id_copy(offset(j)).start()
        return carry

    lax.fori_loop(0, n - 1, send_ids, 0)

    own_ids = pltpu.make_async_copy(ids_out.at[me], ids_in.at[me], smem_sem)
    own_ids.start()
    table_copy.wait()
    tab32[pl.ds(zero_row, 8), :] = jnp.zeros((8, width), F32)
    step = 256

    def widen(i, carry):
        for t in range(tabs):
            base = pl.multiple_of(i * step, step)
            tab32[pl.ds(t * vocab + base, step), :] = tab16[t, pl.ds(base, step), :].astype(F32)
        return carry

    lax.fori_loop(0, vocab // step, widen, 0)

    def pool(source, store):
        def one_table(t, carry):
            at_table = pl.multiple_of(t * most, most)
            for r in range(most):
                total = None
                for p in range(pooling):
                    row = tab32[pl.ds(ids_in[source, t, r * pooling + p], 1), :]
                    total = row if total is None else total + row
                pooled[pl.ds(at_table + r, 1), :] = total
            return carry

        lax.fori_loop(0, tabs, one_table, 0)
        store(pooled[...].astype(BF16))

    def row_copy(peer):
        return pltpu.make_async_remote_copy(
            src_ref=staging.at[peer], dst_ref=rows_ref.at[me],
            send_sem=row_send.at[peer], recv_sem=row_recv.at[me],
            device_id={"dev": peer},
        )

    def serve(j, carry):
        peer = lax.rem(me + offset(j), n)
        id_arrival(peer).wait_recv()

        def store(value):
            staging[peer] = value

        pool(peer, store)
        row_copy(peer).start()
        return carry

    lax.fori_loop(0, n - 1, serve, 0)

    own_ids.wait()

    def store_own(value):
        rows_ref[me] = value

    pool(me, store_own)
    select_samples(most, inv_ref, order_ref, counts_ref, compress_ref, sel, spread_c, mask)

    def finish(i, carry):
        peer = lax.rem(me + i, n)
        id_copy(i).wait_send()
        row_copy(peer).wait_send()
        pltpu.make_async_remote_copy(
            src_ref=staging.at[peer], dst_ref=rows_ref.at[peer],
            send_sem=row_send.at[peer], recv_sem=row_recv.at[peer],
            device_id={"dev": peer},
        ).wait_recv()
        return carry

    lax.fori_loop(1, n, finish, 0)


def exchange(n, most, bags, tables, inv, order, counts, compress):
    tabs, vocab, width = tables.shape
    spread, slots = bags.shape
    block = tabs * most
    total, samples, mixes = n * block, inv.shape[1], compress.shape[0]
    vmem = pl.BlockSpec(memory_space=pltpu.VMEM)
    smem = pl.BlockSpec(memory_space=pltpu.SMEM)
    return pl.pallas_call(
        functools.partial(exchange_kernel, n, most),
        out_shape=[
            jax.ShapeDtypeStruct((n, block, width), BF16),
            jax.ShapeDtypeStruct((samples, total), BF16),
            jax.ShapeDtypeStruct((mixes, total), F32),
            jax.ShapeDtypeStruct((total, samples), F32),
        ],
        in_specs=[vmem, pl.BlockSpec(memory_space=pl.ANY), vmem, smem, smem, vmem],
        out_specs=[vmem] * 4,
        scratch_shapes=[
            pltpu.VMEM(tables.shape, BF16),
            pltpu.VMEM((tabs * vocab + 8, width), F32),
            pltpu.VMEM((n, tabs, spread), jnp.int32),
            pltpu.SMEM((n, tabs, spread), jnp.int32),
            pltpu.VMEM((block, width), F32),
            pltpu.VMEM((n, block, width), BF16),
            pltpu.SemaphoreType.DMA,
            pltpu.SemaphoreType.DMA((n,)),
            pltpu.SemaphoreType.DMA((n,)),
            pltpu.SemaphoreType.DMA,
            pltpu.SemaphoreType.DMA((n,)),
            pltpu.SemaphoreType.DMA((n,)),
        ],
        compiler_params=pltpu.CompilerParams(
            collective_id=0, has_side_effects=True, vmem_limit_bytes=50 << 20
        ),
        name="exchange",
    )(bags, tables, inv, order, counts, compress)


def interact_kernel(
    rows_ref, sel, spread_c, mask, order_ref, weight_ref, bias_ref, out_ref, mixed, pairs,
):
    mixes, total = spread_c.shape
    samples = mask.shape[1]
    width = rows_ref.shape[1]
    features = order_ref.shape[0]
    most = total // features
    per = 8
    span = per * most
    deep = min(total, 2048)

    def mix(k, carry):
        acc = jnp.zeros((samples, width), F32)

        def part(q, acc):
            columns = pl.ds(pl.multiple_of(q * deep, deep), deep)
            scaled = sel[:, columns] * spread_c[pl.ds(k, 1), columns].astype(BF16)
            return acc + jnp.dot(scaled, rows_ref[columns, :], preferred_element_type=F32)

        if total == deep:
            acc = part(0, acc)
        else:
            acc = lax.fori_loop(0, total // deep, part, acc)
        mixed[pl.ds(pl.multiple_of(k * samples, samples), samples), :] = acc.astype(BF16)
        return carry

    lax.fori_loop(0, mixes, mix, 0)

    pair = 2

    def inner(j, carry):
        c8, kp = j // (mixes // pair), j % (mixes // pair)
        wanted = mixed[pl.ds(pl.multiple_of(kp * pair * samples, samples), pair * samples), :]
        for i in range(per):
            c = c8 * per + i
            at = pl.ds(pl.multiple_of(c * span, span), span)
            product = lax.dot_general(
                rows_ref[at, :], wanted, (((1,), (1,)), ((), ())), preferred_element_type=F32
            )
            chosen = mask[at, :]
            for h in range(pair):
                kept = product[:, h * samples:(h + 1) * samples] * chosen
                summed = jnp.sum(kept.reshape(per, most, samples), axis=1)
                for s in range(per):
                    f = order_ref[c * per + s]
                    pairs[pl.ds(f * mixes + kp * pair + h, 1), :] = summed[s:s + 1, :]
        return carry

    lax.fori_loop(0, features // (per * per) * (mixes // pair), inner, 0)

    depth = min(features * mixes, 1024)
    hidden = jnp.zeros(out_ref.shape, F32) + bias_ref[...]

    def top(q, hidden):
        at = pl.ds(pl.multiple_of(q * depth, depth), depth)
        return hidden + lax.dot_general(
            pairs[at, :].astype(BF16), weight_ref[at, :], (((0,), (0,)), ((), ())),
            preferred_element_type=F32,
        )

    if depth == features * mixes:
        hidden = top(0, hidden)
    else:
        hidden = lax.fori_loop(0, features * mixes // depth, top, hidden)
    out_ref[...] = jnp.maximum(hidden, 0.0).astype(BF16)


def interact(rows, sel, spread_c, mask, order, weight, bias):
    mixes, total = spread_c.shape
    samples, features, width = mask.shape[1], order.shape[0], rows.shape[1]
    held = rows.size + weight.size + samples * total + 2 * (mixes + samples) * total
    held += mixes * samples * width + 2 * features * mixes * samples
    vmem = pl.BlockSpec(memory_space=pltpu.VMEM)
    smem = pl.BlockSpec(memory_space=pltpu.SMEM)
    return pl.pallas_call(
        interact_kernel,
        out_shape=jax.ShapeDtypeStruct((samples, weight.shape[1]), BF16),
        in_specs=[vmem, vmem, vmem, vmem, smem, vmem, vmem],
        out_specs=vmem,
        scratch_shapes=[
            pltpu.VMEM((mixes * samples, width), BF16),
            pltpu.VMEM((features * mixes, samples), F32),
        ],
        compiler_params=pltpu.CompilerParams(vmem_limit_bytes=min(60 << 20, (8 << 20) + 3 * held)),
        name="interact",
    )(rows, sel, spread_c, mask, order, weight, bias)


def shards(
    n, tables, bag_rows, bag_lengths, row_counts, inverse, table_order, compress, top_weight, top_bias
):
    _, slots, most, pooling = bag_rows.shape
    tabs, vocab, width = tables.shape
    local = (jnp.arange(slots, dtype=jnp.int32) % tabs) * vocab
    active = jnp.arange(pooling, dtype=jnp.int32)[:, None] < bag_lengths[0].T[:, None, :]
    index = jnp.where(active, bag_rows[0].transpose(1, 2, 0) + local, tabs * vocab)
    rows, sel, spread_c, mask = exchange(
        n, most, index.reshape(most * pooling, slots), tables,
        inverse.T, table_order, row_counts[0], compress,
    )
    return interact(
        rows.reshape(slots * most, width), sel, spread_c, mask, table_order,
        top_weight, top_bias.reshape(1, -1),
    )


def solution(mesh):
    return jax.shard_map(
        functools.partial(shards, mesh.shape["dev"]),
        mesh=mesh,
        in_specs=(
            P("dev", None, None),
            P(("rep", "dev"), None, None, None),
            P(("rep", "dev"), None, None),
            P(("rep", "dev"), None),
            P(("rep", "dev"), None),
            P(),
            P(),
            P(),
            P(),
        ),
        out_specs=P(("rep", "dev"), None),
        check_vma=False,
    )
```
